512 devices in a mesh: gx: 8 (over z_lo, core), gy: 8 (over y), gz: 8 (over x, z_hi).
Axes of the slice: x: 4, y: 8, z: 8 (z_hi: 2, z_lo: 4; z = z_hi * 4 + z_lo), core: 2. Of those that a mesh axis runs over, the one named last changes fastest.
Arguments:
- head_inputs: bfloat16 [131072, 2048], P(('gx', 'gy', 'gz')), may hold values from -6 to 6
- step_raw: float32 [131072, 32], P(('gx', 'gy', 'gz')), may hold values from -4 to 4
- state_in: bfloat16 [131072, 128], P(('gx', 'gy', 'gz')), may hold values from -0.119628906 to 0.119628906
- state_out: bfloat16 [131072, 128], P(('gx', 'gy', 'gz')), may hold values from -0.119628906 to 0.119628906
- decay_log: float32 [32], replicated, may hold values from -13.5 to -3
- step_bias: float32 [32], replicated, may hold values from -1 to 0.5
- skip_gain: float32 [32], replicated, may hold values from 0.5 to 1.5
- checkpoints: bfloat16 [512, 32, 64, 128], P(('gx', 'gy'), None, 'gz'), may hold values from -6 to 6
- out_grad: bfloat16 [131072, 2048], P(('gx', 'gy', 'gz')), may hold values from -6 to 6
Outputs:
- input_grad: bfloat16 [131072, 2048], P(('gx', 'gy', 'gz'))
- step_grad: float32 [131072, 32], P(('gx', 'gy', 'gz'))
- state_in_grad: float32 [131072, 128], P(('gx', 'gy', 'gz'))
- state_out_grad: float32 [131072, 128], P(('gx', 'gy', 'gz'))
- decay_log_grad: float32 [32], replicated
- step_bias_grad: float32 [32], replicated
- skip_gain_grad: float32 [32], replicated
The draws below stay inside these ranges and needn't reach their ends.
All inputs are finite; a program needn't handle non-finite values.
Results may differ from the reference program's by a relative error of at most 0.00065.
Values may be sent and summed in bfloat16 or wider, within the bound.
A program may use at most 128 MiB of HBM per device.

```python
import math
import jax
import jax.numpy as jnp
from jax import lax

HEADS = 32
HEAD_DIM = 64
STATE = 128
SPAN = 256
SPANS = 512
TOKENS = 131072


def draw_decay_log(key, part):
    first, second, third = jax.random.split(key, 3)
    share = 0.5
    keeping = jax.random.uniform(first, (HEADS,), jnp.float32) < share
    keep_low = max(math.log(0.5 / TOKENS), -13.5)
    keep_high = math.log(3.3 / TOKENS)
    quick_low = math.log(1.0 / (2.8 * SPAN))
    slow = jax.random.uniform(second, (HEADS,), jnp.float32, keep_low, keep_high)
    quick = jax.random.uniform(third, (HEADS,), jnp.float32, quick_low, -3.0)
    return jnp.where(keeping, slow, quick)


def levels(own_key, shape, shards, smallest, top_value):
    factor_of, own = 1.0, jax.random.fold_in(own_key, 6)
    for axis_at, shards_of in shards:
        draws = jnp.exp(jax.random.uniform(jax.random.fold_in(own, axis_at), (shards_of,), jnp.float32, smallest / len(shards), top_value / len(shards)))
        factor_of = factor_of * jnp.repeat(draws, shape[axis_at] // shards_of).reshape([-1 if axis == axis_at else 1 for axis in range(len(shape))])
    return factor_of


def bell_draw(stream_key, extent, spread, reach, cuts=(), dtype=jnp.bfloat16):
    values = jax.random.normal(stream_key, extent, jnp.float32) * spread
    if len(cuts) > 0:
        values = levels(stream_key, extent, cuts, -0.22, 0.18) * values
    return jnp.clip(values, min=-reach, max=reach).astype(dtype)


def setup_inputs(seed: int = 0) -> dict:
    keys = jax.random.split(jax.random.key(seed), 10)
    return {
        "head_inputs": bell_draw(keys[0], (TOKENS, HEADS * HEAD_DIM), 1.0, 6.0, ((0, 512),)),
        "step_raw": bell_draw(keys[1], (TOKENS, HEADS), 1.0, 4.0, ((0, 512),), jnp.float32),
        "state_in": bell_draw(keys[2], (TOKENS, STATE), 0.02, 0.119628906, ((0, 512),)),
        "state_out": bell_draw(keys[3], (TOKENS, STATE), 0.02, 0.119628906, ((0, 512),)),
        "decay_log": draw_decay_log(jax.random.fold_in(keys[9], 71), 0),
        "step_bias": jnp.clip(jax.random.uniform(keys[5], (HEADS,), jnp.float32, -1.0, 0.5), -1.0, 0.5),
        "skip_gain": jnp.clip(jax.random.uniform(keys[6], (HEADS,), jnp.float32, 0.5, 1.5), 0.5, 1.5),
        "checkpoints": bell_draw(keys[7], (SPANS, HEADS, HEAD_DIM, STATE), 1.0, 6.0, ((0, 64), (2, 8))),
        "out_grad": bell_draw(keys[8], (TOKENS, HEADS * HEAD_DIM), 1.0, 6.0, ((0, 512),)),
    }


highest = lax.Precision.HIGHEST

def block_forward(inputs, raw, b_mat, c_mat, decay_log, bias, skip, start):
    step = jax.nn.softplus(raw + bias)
    cum = jnp.cumsum(step * -jnp.exp(decay_log), axis=0)
    length = inputs.shape[0]
    rows = lax.broadcasted_iota(jnp.int32, (length, length), 0)
    cols = lax.broadcasted_iota(jnp.int32, (length, length), 1)
    lower = rows >= cols
    scores = jnp.dot(c_mat, b_mat.T, precision=highest)
    ctrans = cum.T
    gap = ctrans[:, :, None] - ctrans[:, None, :]
    mix = jnp.where(lower, jnp.exp(jnp.where(lower, gap, 0.0)), 0.0) * scores * step.T[:, None, :]
    inner = jnp.einsum('hts,shp->thp', mix, inputs, precision=highest)
    carried = jnp.einsum('tn,hpn->thp', c_mat, start, precision=highest) * jnp.exp(cum)[:, :, None]
    result = inner + carried + skip[None, :, None] * inputs
    tail = jnp.exp(cum[-1][None, :] - cum) * step
    final = jnp.exp(cum[-1])[:, None, None] * start + jnp.einsum('sh,shp,sn->hpn', tail, inputs, b_mat, precision=highest)
    return (result, final)

def span_forward(inputs, raw, b_mat, c_mat, decay_log, bias, skip, start):
    length, heads = raw.shape
    width = inputs.shape[1] // heads
    states = start.shape[2]
    block = min(8, heads)
    blocks = heads // block
    grouped = inputs.reshape(length, blocks, block, width).transpose(1, 0, 2, 3)
    raw_g = raw.reshape(length, blocks, block).transpose(1, 0, 2)

    def one_block(items):
        return block_forward(items[0], items[1], b_mat, c_mat, items[2], items[3], items[4], items[5])
    result, final = lax.map(one_block, (grouped, raw_g, decay_log.reshape(blocks, block), bias.reshape(blocks, block), skip.reshape(blocks, block), start.reshape(blocks, block, width, states)))
    result = result.transpose(1, 0, 2, 3).reshape(length, heads * width)
    return (result, final.reshape(heads, width, states))

def reference(head_inputs, step_raw, state_in, state_out, decay_log, step_bias, skip_gain, checkpoints, out_grad):
    spans = checkpoints.shape[0]
    heads = decay_log.shape[0]
    wide = head_inputs.shape[1]
    states = state_in.shape[1]
    items = (head_inputs.reshape(spans, SPAN, wide), step_raw.reshape(spans, SPAN, heads), state_in.reshape(spans, SPAN, states), state_out.reshape(spans, SPAN, states), checkpoints, out_grad.reshape(spans, SPAN, wide))

    def backward(carry, item):
        later, g_decay, g_bias, g_skip = carry
        inputs, raw, b_mat, c_mat, start, grad = item
        _, pull = jax.vjp(span_forward, inputs.astype(jnp.float32), raw, b_mat.astype(jnp.float32), c_mat.astype(jnp.float32), decay_log, step_bias, skip_gain, start.astype(jnp.float32))
        grads = pull((grad.astype(jnp.float32), later))
        new_carry = (grads[7], g_decay + grads[4], g_bias + grads[5], g_skip + grads[6])
        return (new_carry, (grads[0].astype(jnp.bfloat16), grads[1], grads[2], grads[3]))
    zeros_state = jnp.zeros(checkpoints.shape[1:], jnp.float32)
    zeros_head = jnp.zeros((heads,), jnp.float32)
    init = (zeros_state, zeros_head, zeros_head, zeros_head)
    final, outs = lax.scan(backward, init, items, reverse=True)
    input_grad = outs[0].reshape(spans * SPAN, wide)
    step_grad = outs[1].reshape(spans * SPAN, heads)
    state_in_grad = outs[2].reshape(spans * SPAN, states)
    state_out_grad = outs[3].reshape(spans * SPAN, states)
    return (input_grad, step_grad, state_in_grad, state_out_grad, final[1], final[2], final[3])
```

```python
import jax
import jax.numpy as jnp
from jax import lax
from jax.experimental import pallas as pl
from jax.experimental.pallas import tpu as pltpu
from jax.sharding import Mesh
from jax.sharding import PartitionSpec as P

F32, BF16 = jnp.float32, jnp.bfloat16
HEADS, WIDTH, STATES, SPAN = 32, 64, 128, 256
CHUNK = 256
CHUNKS = HEADS * WIDTH // CHUNK


def iota(shape, axis):
    return lax.broadcasted_iota(jnp.int32, shape, axis)


def mm(a, b, ca=1, cb=0):
    return lax.dot_general(a, b, (((ca,), (cb,)), ((), ())), preferred_element_type=F32)


def two(v):
    hi = v.astype(BF16)
    return hi, (v - hi.astype(F32)).astype(BF16)


def three(v):
    hi = v.astype(BF16)
    rest = v - hi.astype(F32)
    mid = rest.astype(BF16)
    return hi, mid, (rest - mid.astype(F32)).astype(BF16)


def lanes(v):
    hi = v.astype(BF16).astype(F32)
    rest = v - hi
    mid = rest.astype(BF16).astype(F32)
    at = iota(v.shape, 1) // HEADS
    return jnp.where(at == 0, hi, jnp.where(at == 1, mid, jnp.where(at == 2, rest - mid, 0.0))).astype(BF16)


def spread_matrix(j):
    row, col = iota((128, CHUNK), 0), iota((128, CHUNK), 1)
    return jnp.where(row % HEADS == col // WIDTH + j * (CHUNK // WIDTH), 1.0, 0.0).astype(BF16)


def gather_matrix(j):
    row, col = iota((CHUNK, 128), 0), iota((CHUNK, 128), 1)
    return jnp.where(col % HEADS == row // WIDTH + j * (CHUNK // WIDTH), 1.0, 0.0).astype(BF16)


def seg(v, ones):
    a, b, c = three(v)
    return mm(a, ones) + mm(b, ones) + mm(c, ones)


def tri(lower):
    r, c = iota((SPAN, SPAN), 0), iota((SPAN, SPAN), 1)
    return jnp.where((r >= c) if lower else (r <= c), 1.0, 0.0).astype(BF16)


def scalars(raw4, bias4, decay4):
    z = raw4 + bias4
    step = jnp.maximum(z, 0.0) + jnp.log1p(jnp.exp(-jnp.abs(z)))
    rate = jnp.exp(decay4)
    low = tri(True)
    a, b, c = three(step * -rate)
    cum = mm(low, a) + mm(low, b) + mm(low, c)
    return z, step, rate, cum


def first_kernel(raw_ref, bias_ref, decay_ref, g_ref, c_ref, term_ref, decays_ref, e_ref):
    j = pl.program_id(0)

    @pl.when(j == 0)
    def _():
        _, _, _, cum = scalars(raw_ref[...], bias_ref[...], decay_ref[...])
        e = jnp.exp(cum)
        e_ref[...] = lanes(e)
        decays_ref[...] = jnp.broadcast_to(e[SPAN - 1 :, :], (8, 128))

    wide = mm(e_ref[...], spread_matrix(j))
    hi, lo = two(g_ref[...].astype(F32) * wide)
    c = c_ref[...]
    term_ref[...] = mm(hi, c, 0, 0) + mm(lo, c, 0, 0)


def first(raw4, bias4, decay4, g, c):
    return pl.pallas_call(
        first_kernel,
        grid=(CHUNKS,),
        out_shape=(
            jax.ShapeDtypeStruct((HEADS * WIDTH, STATES), F32),
            jax.ShapeDtypeStruct((8, 128), F32),
        ),
        in_specs=[
            pl.BlockSpec((SPAN, 128), lambda j: (0, 0)),
            pl.BlockSpec((1, 128), lambda j: (0, 0)),
            pl.BlockSpec((1, 128), lambda j: (0, 0)),
            pl.BlockSpec((SPAN, CHUNK), lambda j: (0, j)),
            pl.BlockSpec((SPAN, STATES), lambda j: (0, 0)),
        ],
        out_specs=(
            pl.BlockSpec((CHUNK, STATES), lambda j: (j, 0)),
            pl.BlockSpec((8, 128), lambda j: (0, 0)),
        ),
        scratch_shapes=[pltpu.VMEM((SPAN, 128), BF16)],
        name="first",
    )(raw4, bias4, decay4, g, c)


def second_kernel(
    raw_ref, bias_ref, decay_ref, skip_ref, x_ref, g_ref, b_ref, c_ref, h_ref, later_ref,
    dx_ref, draw_ref, db_ref, dc_ref, par_ref,
    e_ref, f_ref, small, sh, sl, th, tl, ds_ref, a_acc, r_acc, row_acc,
):
    j = pl.program_id(0)

    @pl.when(j == 0)
    def _():
        z, step, rate, cum = scalars(raw_ref[...], bias_ref[...], decay_ref[...])
        back = jnp.exp(-cum)
        e_ref[...] = lanes(jnp.exp(cum))
        f_ref[...] = lanes(back * step)
        small[0], small[1], small[2] = step, back, back * step
        r, c = iota((SPAN, SPAN), 0), iota((SPAN, SPAN), 1)
        s = jnp.where(r >= c, mm(c_ref[...], b_ref[...], 1, 1), 0.0)
        sh[...], sl[...] = two(s)
        t = jnp.where(r <= c, mm(b_ref[...], c_ref[...], 1, 1), 0.0)
        th[...], tl[...] = two(t)
        for ref in (ds_ref, a_acc, r_acc, row_acc, db_ref, dc_ref):
            ref[...] = jnp.zeros_like(ref)

    spread, ones = spread_matrix(j), gather_matrix(j)
    e = mm(e_ref[...], spread)
    f = mm(f_ref[...], spread)
    end = e[SPAN - 1 :, :]
    skip = mm(lanes(jnp.broadcast_to(skip_ref[...], (8, 128))), spread)[:1, :]
    x_bf, g_bf, h = x_ref[...], g_ref[...], h_ref[...]
    x, g = x_bf.astype(F32), g_bf.astype(F32)
    gw, xw = g * e, x * f
    gh, gl = two(gw)
    xh, xl = two(xw)
    later = later_ref[...]
    lh, ll = two(later)
    y = mm(sh[...], xh) + mm(sl[...], xh) + mm(sh[...], xl) + mm(c_ref[...], h, 1, 1)
    q = (mm(b_ref[...], lh, 1, 1) + mm(b_ref[...], ll, 1, 1)) * end
    zq = mm(th[...], gh) + mm(tl[...], gh) + mm(th[...], gl) + q
    dx_ref[...] = (f * zq + skip * g).astype(BF16)
    a_acc[...] += seg(gw * y, ones)
    r_acc[...] += seg(x * zq, ones)
    ds_ref[...] += mm(gh, xh, 1, 1) + mm(gl, xh, 1, 1) + mm(gh, xl, 1, 1)
    dc_ref[...] += mm(gh, h) + mm(gl, h)
    eh, el = two(xw * end)
    db_ref[...] += mm(eh, lh) + mm(el, lh) + mm(eh, ll)
    p0, p1, p2 = three(h.astype(F32) * later)
    one8 = jnp.ones((8, STATES), BF16)
    dots = mm(one8, p0, 1, 1) + mm(one8, p1, 1, 1) + mm(one8, p2, 1, 1)
    at_end = jnp.sum(xw * q, axis=0, keepdims=True) + end * dots
    direct = jnp.sum(x * g, axis=0, keepdims=True)
    rows = jnp.where(iota((8, CHUNK), 0) == 0, at_end, direct)
    row_acc[...] += seg(rows, ones)

    @pl.when(j == CHUNKS - 1)
    def _():
        r, c = iota((SPAN, SPAN), 0), iota((SPAN, SPAN), 1)
        dh, dl = two(jnp.where(r >= c, ds_ref[...], 0.0))
        dc_ref[...] += mm(dh, b_ref[...]) + mm(dl, b_ref[...])
        db_ref[...] += mm(dh, c_ref[...], 0, 0) + mm(dl, c_ref[...], 0, 0)
        z = raw_ref[...] + bias_ref[...]
        rate = jnp.exp(decay_ref[...])
        step, back, ff = small[0], small[1], small[2]
        last = iota((SPAN, 128), 0) == SPAN - 1
        dcum = a_acc[...] - ff * r_acc[...] + jnp.where(last, row_acc[0:1, :], 0.0)
        up = tri(False)
        q0, q1, q2 = three(dcum)
        rc = mm(up, q0) + mm(up, q1) + mm(up, q2)
        draw = (back * r_acc[...] - rate * rc) / (1.0 + jnp.exp(-z))
        draw_ref[...] = draw[:, :HEADS]
        pd = jnp.sum(rc * step, axis=0, keepdims=True) * -rate
        pb = jnp.sum(draw, axis=0, keepdims=True)
        lane = iota((1, 128), 1) // HEADS
        par_ref[...] = jnp.where(lane == 0, pd, jnp.where(lane == 1, pb, jnp.where(lane == 2, row_acc[1:2, :], 0.0)))


def second(raw4, bias4, decay4, skip4, x, g, b, c, h, later):
    whole = lambda *shape: pl.BlockSpec(shape, lambda j: (0,) * len(shape))
    cols = pl.BlockSpec((SPAN, CHUNK), lambda j: (0, j))
    rows = pl.BlockSpec((CHUNK, STATES), lambda j: (j, 0))
    return pl.pallas_call(
        second_kernel,
        grid=(CHUNKS,),
        out_shape=(
            jax.ShapeDtypeStruct((SPAN, HEADS * WIDTH), BF16),
            jax.ShapeDtypeStruct((SPAN, HEADS), F32),
            jax.ShapeDtypeStruct((SPAN, STATES), F32),
            jax.ShapeDtypeStruct((SPAN, STATES), F32),
            jax.ShapeDtypeStruct((1, 128), F32),
        ),
        in_specs=[whole(SPAN, 128), whole(1, 128), whole(1, 128), whole(1, 128), cols, cols,
                  whole(SPAN, STATES), whole(SPAN, STATES), rows, rows],
        out_specs=(cols, whole(SPAN, HEADS), whole(SPAN, STATES), whole(SPAN, STATES), whole(1, 128)),
        scratch_shapes=[
            pltpu.VMEM((SPAN, 128), BF16), pltpu.VMEM((SPAN, 128), BF16), pltpu.VMEM((3, SPAN, 128), F32),
            pltpu.VMEM((SPAN, SPAN), BF16), pltpu.VMEM((SPAN, SPAN), BF16),
            pltpu.VMEM((SPAN, SPAN), BF16), pltpu.VMEM((SPAN, SPAN), BF16),
            pltpu.VMEM((SPAN, SPAN), F32), pltpu.VMEM((SPAN, 128), F32), pltpu.VMEM((SPAN, 128), F32),
            pltpu.VMEM((8, 128), F32),
        ],
        name="second",
    )(raw4, bias4, decay4, skip4, x, g, b, c, h, later)


GZ = ("gz_0", "gz_1")
GX_GY = ("gx_0", "gx_1", "gy")
GX_GY_GZ = GX_GY + GZ


def four(a):
    return jnp.tile(a.reshape(-1, HEADS), (1, 4))


def local(x, raw, b, c, decay, bias, skip, checkpoints, g):
    raw4, bias4, decay4, skip4 = four(raw), four(bias), four(decay), four(skip)
    start = lax.all_to_all(checkpoints, GZ, split_axis=0, concat_axis=2, tiled=True)[0]
    term, decays = first(raw4, bias4, decay4, g, c)
    group = lax.axis_size(GZ)
    part = HEADS // group
    every = lax.all_gather(decays[0, :HEADS], GX_GY_GZ)
    got = lax.all_to_all(term.reshape(group, part, WIDTH, STATES), GZ, split_axis=0, concat_axis=0, tiled=True)
    mine = lax.dynamic_slice_in_dim(every, lax.axis_index(GZ) * part, part, axis=1)
    mine = mine.reshape(-1, group, part)
    own = lax.dynamic_index_in_dim(mine, lax.axis_index(GX_GY), 0, keepdims=False)
    state = jnp.zeros((part, WIDTH, STATES), F32)
    inside = [None] * group
    lead = [None] * group
    keep = jnp.ones((part,), F32)
    for m in reversed(range(group)):
        inside[m], lead[m] = state, keep
        state = got[m] + own[m][:, None, None] * state
        keep = own[m] * keep
    keeps = jnp.prod(mine, axis=1)
    total, reach = state, None
    lengths = [lax.axis_size(a) for a in GX_GY]
    table = keeps.reshape(*lengths, part)
    carry = jnp.zeros_like(state)
    for at in reversed(range(3)):
        axis, n = GX_GY[at], lengths[at]
        index = lax.axis_index(axis)
        pieces = lax.all_gather(total, axis)
        row = table
        for other in range(at):
            row = lax.dynamic_index_in_dim(row, lax.axis_index(GX_GY[other]), 0, keepdims=False)
        row = jnp.prod(row.reshape(n, -1, part), axis=1)
        run, found = jnp.zeros_like(state), jnp.zeros_like(state)
        for i in reversed(range(n)):
            found = jnp.where(i == index, run, found)
            run = pieces[i] + row[i][:, None, None] * run
        if reach is None:
            carry, total = found, run
            reach = jnp.ones((part,), F32)
        else:
            carry, total = carry + reach[:, None, None] * found, run
        before = jnp.where((jnp.arange(n) > index)[:, None], row, 1.0)
        reach = reach * jnp.prod(before, axis=0)
    back = jnp.stack([inside[m] + lead[m][:, None, None] * carry for m in range(group)])
    later = lax.all_to_all(back, GZ, split_axis=0, concat_axis=0, tiled=True).reshape(HEADS * WIDTH, STATES)
    dx, draw, db, dc, params = second(
        raw4, bias4, decay4, skip4, x, g, b, c, start.reshape(HEADS * WIDTH, STATES), later
    )
    sums = lax.psum(params[0], GX_GY_GZ)
    return dx, draw, db, dc, sums[:HEADS], sums[HEADS : 2 * HEADS], sums[2 * HEADS : 3 * HEADS]


def solution(mesh):
    torus = Mesh(
        mesh.devices.reshape(4, 2, mesh.shape["gy"], 4, 2), ("gx_0", "gx_1", "gy", "gz_0", "gz_1")
    )
    wide = P(GX_GY_GZ, None)
    return jax.shard_map(
        local,
        mesh=torus,
        in_specs=(wide, wide, wide, wide, P(), P(), P(), P(GX_GY, None, GZ, None), wide),
        out_specs=(wide, wide, wide, wide, P(), P(), P()),
        check_vma=False,
    )
```

```python
import jax
import jax.numpy as jnp
from jax import lax
from jax.experimental import pallas as pl
from jax.experimental.pallas import tpu as pltpu
from jax.sharding import Mesh
from jax.sharding import PartitionSpec as P

F32, BF16 = jnp.float32, jnp.bfloat16
HEADS, WIDTH, STATES, SPAN = 32, 64, 128, 256
CHUNK = 256
CHUNKS = HEADS * WIDTH // CHUNK


def iota(shape, axis):
    return lax.broadcasted_iota(jnp.int32, shape, axis)


def mm(a, b, ca=1, cb=0):
    return lax.dot_general(a, b, (((ca,), (cb,)), ((), ())), preferred_element_type=F32)


def two(v):
    hi = v.astype(BF16)
    return hi, (v - hi.astype(F32)).astype(BF16)


def three(v):
    hi = v.astype(BF16)
    rest = v - hi.astype(F32)
    mid = rest.astype(BF16)
    return hi, mid, (rest - mid.astype(F32)).astype(BF16)


def lanes(v):
    hi = v.astype(BF16).astype(F32)
    rest = v - hi
    mid = rest.astype(BF16).astype(F32)
    at = iota(v.shape, 1) // HEADS
    return jnp.where(at == 0, hi, jnp.where(at == 1, mid, jnp.where(at == 2, rest - mid, 0.0))).astype(BF16)


def spread_matrix(j):
    row, col = iota((128, CHUNK), 0), iota((128, CHUNK), 1)
    return jnp.where(row % HEADS == col // WIDTH + j * (CHUNK // WIDTH), 1.0, 0.0).astype(BF16)


def gather_matrix(j):
    row, col = iota((CHUNK, 128), 0), iota((CHUNK, 128), 1)
    return jnp.where(col % HEADS == row // WIDTH + j * (CHUNK // WIDTH), 1.0, 0.0).astype(BF16)


def seg(v, ones):
    a, b, c = three(v)
    return mm(a, ones) + mm(b, ones) + mm(c, ones)


def tri(lower):
    r, c = iota((SPAN, SPAN), 0), iota((SPAN, SPAN), 1)
    return jnp.where((r >= c) if lower else (r <= c), 1.0, 0.0).astype(BF16)


def scalars(raw4, bias4, decay4):
    z = raw4 + bias4
    step = jnp.maximum(z, 0.0) + jnp.log1p(jnp.exp(-jnp.abs(z)))
    rate = jnp.exp(decay4)
    low = tri(True)
    a, b, c = three(step * -rate)
    cum = mm(low, a) + mm(low, b) + mm(low, c)
    return z, step, rate, cum


def first_kernel(raw_ref, par_ref, g_ref, c_ref, term_ref, e_ref):
    j = pl.program_id(0)

    @pl.when(j == 0)
    def _():
        _, _, _, cum = scalars(raw_ref[...], par_ref[0:1, :], par_ref[1:2, :])
        e_ref[...] = lanes(jnp.exp(cum))

    wide = mm(e_ref[...], spread_matrix(j))
    hi, lo = two(g_ref[...].astype(F32) * wide)
    c = c_ref[...]
    term_ref[0, :CHUNK] = mm(hi, c, 0, 0) + mm(lo, c, 0, 0)
    row, lane = iota((8, 128), 0), iota((8, 128), 1)
    ends = jnp.where(lane % HEADS == row + j * (CHUNK // WIDTH), e_ref[SPAN - 1 :, :].astype(F32), 0.0)
    term_ref[0, CHUNK:] = mm(ends.astype(BF16), jnp.ones((128, STATES), BF16))


def first(raw4, par4, g, c):
    return pl.pallas_call(
        first_kernel,
        grid=(CHUNKS,),
        out_shape=jax.ShapeDtypeStruct((CHUNKS, CHUNK + 8, STATES), F32),
        in_specs=[
            pl.BlockSpec((SPAN, 128), lambda j: (0, 0)),
            pl.BlockSpec((3, 128), lambda j: (0, 0)),
            pl.BlockSpec((SPAN, CHUNK), lambda j: (0, j)),
            pl.BlockSpec((SPAN, STATES), lambda j: (0, 0)),
        ],
        out_specs=pl.BlockSpec((1, CHUNK + 8, STATES), lambda j: (j, 0, 0)),
        scratch_shapes=[pltpu.VMEM((SPAN, 128), BF16)],
        name="first",
    )(raw4, par4, g, c)


def second_kernel(
    raw_ref, par_ref, x_ref, g_ref, b_ref, c_ref, h_ref, later_ref,
    dx_ref, draw_ref, db_ref, dc_ref, sums_ref,
    e_ref, f_ref, small, sh, sl, th, tl, ds_ref, a_acc, r_acc, row_acc,
):
    j = pl.program_id(0)

    @pl.when(j == 0)
    def _():
        z, step, rate, cum = scalars(raw_ref[...], par_ref[0:1, :], par_ref[1:2, :])
        back = jnp.exp(-cum)
        e_ref[...] = lanes(jnp.exp(cum))
        f_ref[...] = lanes(back * step)
        small[0], small[1], small[2] = step, back, back * step
        r, c = iota((SPAN, SPAN), 0), iota((SPAN, SPAN), 1)
        s = jnp.where(r >= c, mm(c_ref[...], b_ref[...], 1, 1), 0.0)
        sh[...], sl[...] = two(s)
        t = jnp.where(r <= c, mm(b_ref[...], c_ref[...], 1, 1), 0.0)
        th[...], tl[...] = two(t)
        for ref in (ds_ref, a_acc, r_acc, row_acc, db_ref, dc_ref):
            ref[...] = jnp.zeros_like(ref)

    spread, ones = spread_matrix(j), gather_matrix(j)
    e = mm(e_ref[...], spread)
    f = mm(f_ref[...], spread)
    end = e[SPAN - 1 :, :]
    skip = mm(lanes(jnp.broadcast_to(par_ref[2:3, :], (8, 128))), spread)[:1, :]
    x_bf, g_bf = x_ref[...], g_ref[...]
    h32 = h_ref[...].astype(F32).transpose(1, 0, 2, 3).reshape(CHUNK, STATES)
    h = h32.astype(BF16)
    x, g = x_bf.astype(F32), g_bf.astype(F32)
    gw, xw = g * e, x * f
    gh, gl = two(gw)
    xh, xl = two(xw)
    later = later_ref[...]
    lh, ll = two(later)
    y = mm(sh[...], xh) + mm(sl[...], xh) + mm(sh[...], xl) + mm(c_ref[...], h, 1, 1)
    q = (mm(b_ref[...], lh, 1, 1) + mm(b_ref[...], ll, 1, 1)) * end
    zq = mm(th[...], gh) + mm(tl[...], gh) + mm(th[...], gl) + q
    dx_ref[...] = (f * zq + skip * g).astype(BF16)
    a_acc[...] += seg(gw * y, ones)
    r_acc[...] += seg(x * zq, ones)
    ds_ref[...] += mm(gh, xh, 1, 1) + mm(gl, xh, 1, 1) + mm(gh, xl, 1, 1)
    dc_ref[...] += mm(gh, h) + mm(gl, h)
    eh, el = two(xw * end)
    db_ref[...] += mm(eh, lh) + mm(el, lh) + mm(eh, ll)
    p0, p1, p2 = three(h32 * later)
    one8 = jnp.ones((8, STATES), BF16)
    dots = mm(one8, p0, 1, 1) + mm(one8, p1, 1, 1) + mm(one8, p2, 1, 1)
    at_end = jnp.sum(xw * q, axis=0, keepdims=True) + end * dots
    direct = jnp.sum(x * g, axis=0, keepdims=True)
    rows = jnp.where(iota((8, CHUNK), 0) == 0, at_end, direct)
    row_acc[...] += seg(rows, ones)

    @pl.when(j == CHUNKS - 1)
    def _():
        r, c = iota((SPAN, SPAN), 0), iota((SPAN, SPAN), 1)
        dh, dl = two(jnp.where(r >= c, ds_ref[...], 0.0))
        dc_ref[...] += mm(dh, b_ref[...]) + mm(dl, b_ref[...])
        db_ref[...] += mm(dh, c_ref[...], 0, 0) + mm(dl, c_ref[...], 0, 0)
        z = raw_ref[...] + par_ref[0:1, :]
        rate = jnp.exp(par_ref[1:2, :])
        step, back, ff = small[0], small[1], small[2]
        last = iota((SPAN, 128), 0) == SPAN - 1
        dcum = a_acc[...] - ff * r_acc[...] + jnp.where(last, row_acc[0:1, :], 0.0)
        up = tri(False)
        q0, q1, q2 = three(dcum)
        rc = mm(up, q0) + mm(up, q1) + mm(up, q2)
        draw = (back * r_acc[...] - rate * rc) / (1.0 + jnp.exp(-z))
        draw_ref[...] = draw[:, :HEADS]
        pd = jnp.sum(rc * step, axis=0, keepdims=True) * -rate
        pb = jnp.sum(draw, axis=0, keepdims=True)
        lane = iota((1, 128), 1) // HEADS
        sums = jnp.where(lane == 0, pd, jnp.where(lane == 1, pb, jnp.where(lane == 2, row_acc[1:2, :], 0.0)))
        sums_ref[...] = jnp.broadcast_to(sums, (8, 128))


def second(raw4, par4, x, g, b, c, h, later):
    whole = lambda *shape: pl.BlockSpec(shape, lambda j: (0,) * len(shape))
    cols = pl.BlockSpec((SPAN, CHUNK), lambda j: (0, j))
    rows = pl.BlockSpec((CHUNK, STATES), lambda j: (j, 0))
    return pl.pallas_call(
        second_kernel,
        grid=(CHUNKS,),
        out_shape=(
            jax.ShapeDtypeStruct((SPAN, HEADS * WIDTH), BF16),
            jax.ShapeDtypeStruct((SPAN, HEADS), F32),
            jax.ShapeDtypeStruct((SPAN, STATES), F32),
            jax.ShapeDtypeStruct((SPAN, STATES), F32),
            jax.ShapeDtypeStruct((8, 128), F32),
        ),
        in_specs=[whole(SPAN, 128), whole(3, 128), cols, cols, whole(SPAN, STATES), whole(SPAN, STATES),
                  pl.BlockSpec((8, CHUNK // WIDTH, 8, STATES), lambda j: (0, j, 0, 0)), rows],
        out_specs=(cols, whole(SPAN, HEADS), whole(SPAN, STATES), whole(SPAN, STATES), whole(8, 128)),
        scratch_shapes=[
            pltpu.VMEM((SPAN, 128), BF16), pltpu.VMEM((SPAN, 128), BF16), pltpu.VMEM((3, SPAN, 128), F32),
            pltpu.VMEM((SPAN, SPAN), BF16), pltpu.VMEM((SPAN, SPAN), BF16),
            pltpu.VMEM((SPAN, SPAN), BF16), pltpu.VMEM((SPAN, SPAN), BF16),
            pltpu.VMEM((SPAN, SPAN), F32), pltpu.VMEM((SPAN, 128), F32), pltpu.VMEM((SPAN, 128), F32),
            pltpu.VMEM((8, 128), F32),
        ],
        name="second",
    )(raw4, par4, x, g, b, c, h, later)


MESH = pl.DeviceIdType.MESH
PART = HEADS // 8
SLICE = PART * WIDTH
PIECE = SLICE // 8


def places():
    zx, zz = lax.axis_index("gz_0"), lax.axis_index("gz_1")
    return zx * 2 + zz, lax.axis_index("gy"), lax.axis_index("gx_0") * 2 + lax.axis_index("gx_1")


def gz_peer(i):
    return {"gz_0": i // 2, "gz_1": i % 2}


def gy_peer(i):
    return {"gy": i}


def gx_peer(i):
    return {"gx_0": i // 2, "gx_1": i % 2}


def greet(groups):
    barrier = pltpu.get_barrier_semaphore()
    for me, peer in groups:
        for d in range(1, 8):
            pl.semaphore_signal(barrier, inc=1, device_id=peer((me + d) % 8), device_id_type=MESH)
    pl.semaphore_wait(barrier, 7 * len(groups))


def send_all(me, peer, src, dst, send, recv, row):
    copies = []
    for d in range(1, 8):
        to = (me + d) % 8
        copy = pltpu.make_async_remote_copy(
            src_ref=src(to), dst_ref=dst.at[me], send_sem=send.at[row, d], recv_sem=recv.at[row, d],
            device_id=peer(to), device_id_type=MESH,
        )
        copy.start()
        copies.append(copy)
    return copies


def wait_all(copies):
    for copy in copies:
        copy.wait()


def by_head(state, keep):
    return (state.reshape(PART, WIDTH, STATES) * keep[:PART][:, None, :]).reshape(SLICE, STATES)


def exchange_kernel(
    term_ref, ckpt_ref, later_ref, start_ref,
    rec1, inside, lead, tot3, rec3, inside3, lead3, tot4, rec4, out5, rec5, out6, send, recv,
):
    gz, gy, gx = places()
    greet(((gz, gz_peer), (gy, gy_peer), (gx, gx_peer)))
    first_way = send_all(gz, gz_peer, lambda to: term_ref.at[to], rec1, send, recv, 0)
    states = send_all(gz, gz_peer, lambda to: ckpt_ref.at[to], start_ref, send, recv, 1)
    rec1[gz] = term_ref[gz]
    start_ref[gz] = ckpt_ref[gz]
    wait_all(first_way)
    run = jnp.zeros((SLICE, STATES), F32)
    keep = jnp.ones((8, STATES), F32)
    for m in reversed(range(8)):
        inside[m] = run
        lead[m] = keep
        own = rec1[m, SLICE:]
        run = rec1[m, :SLICE] + by_head(run, own)
        keep = keep * own
    for i in range(8):
        tot3[i, :PIECE] = run[i * PIECE : (i + 1) * PIECE]
        tot3[i, PIECE:] = jnp.broadcast_to(keep[i // 2 : i // 2 + 1], (8, STATES))
    scatter = send_all(gy, gy_peer, lambda to: tot3.at[to], rec3, send, recv, 2)
    rec3[gy] = tot3[gy]
    wait_all(scatter)
    run = jnp.zeros((PIECE, STATES), F32)
    keep = jnp.ones((8, STATES), F32)
    for m in reversed(range(8)):
        inside3[m] = run
        lead3[m] = keep
        own = rec3[m, PIECE:]
        run = rec3[m, :PIECE] + run * own[:1]
        keep = keep * own
    tot4[:PIECE] = run
    tot4[PIECE:] = keep
    outer = send_all(gx, gx_peer, lambda to: tot4, rec4, send, recv, 3)
    rec4[gx] = tot4[...]
    wait_all(outer)
    run = jnp.zeros((PIECE, STATES), F32)
    carry = run
    for m in reversed(range(8)):
        carry = jnp.where(gx == m, run, carry)
        run = rec4[m, :PIECE] + run * rec4[m, PIECE : PIECE + 1]
    for m in range(8):
        out5[m] = inside3[m] + lead3[m, :1] * carry
    gather = send_all(gy, gy_peer, lambda to: out5.at[to], rec5, send, recv, 4)
    rec5[gy] = out5[gy]
    wait_all(gather)
    carry = rec5[...].reshape(SLICE, STATES)
    for m in range(8):
        out6[m] = inside[m] + by_head(carry, lead[m])
    back = send_all(gz, gz_peer, lambda to: out6.at[to], later_ref, send, recv, 5)
    later_ref[gz] = out6[gz]
    wait_all(states)
    wait_all(back)


def exchange(term, checkpoints):
    vmem = pl.BlockSpec(memory_space=pltpu.VMEM)
    buf = lambda *shape: pltpu.VMEM(shape, F32)
    return pl.pallas_call(
        exchange_kernel,
        out_shape=(
            jax.ShapeDtypeStruct((8, SLICE, STATES), F32),
            jax.ShapeDtypeStruct(checkpoints.shape, BF16),
        ),
        in_specs=[vmem, vmem],
        out_specs=(vmem, vmem),
        scratch_shapes=[
            buf(8, SLICE + 8, STATES), buf(8, SLICE, STATES), buf(8, 8, STATES),
            buf(8, PIECE + 8, STATES), buf(8, PIECE + 8, STATES), buf(8, PIECE, STATES), buf(8, 8, STATES),
            buf(PIECE + 8, STATES), buf(8, PIECE + 8, STATES), buf(8, PIECE, STATES), buf(8, PIECE, STATES),
            buf(8, SLICE, STATES),
            pltpu.SemaphoreType.DMA((6, 8)), pltpu.SemaphoreType.DMA((6, 8)),
        ],
        compiler_params=pltpu.CompilerParams(collective_id=0, has_side_effects=True, vmem_limit_bytes=48 * 2**20),
        name="exchange",
    )(term, checkpoints)


def sum_kernel(par_ref, out_ref, block, rec, send, recv):
    gz, gy, gx = places()
    groups = ((gz, gz_peer), (gy, gy_peer), (gx, gx_peer))
    greet(groups)
    total = par_ref[...]
    for k, (me, peer) in enumerate(groups):
        block[k] = total
        copies = send_all(me, peer, lambda to: block.at[k], rec.at[k], send, recv, k)
        rec[k, me] = total
        wait_all(copies)
        total = rec[k, 0]
        for m in range(1, 8):
            total = total + rec[k, m]
    out_ref[...] = total


def sum_all(params):
    vmem = pl.BlockSpec(memory_space=pltpu.VMEM)
    return pl.pallas_call(
        sum_kernel,
        out_shape=jax.ShapeDtypeStruct((8, 128), F32),
        in_specs=[vmem],
        out_specs=vmem,
        scratch_shapes=[
            pltpu.VMEM((3, 8, 128), F32), pltpu.VMEM((3, 8, 8, 128), F32),
            pltpu.SemaphoreType.DMA((3, 8)), pltpu.SemaphoreType.DMA((3, 8)),
        ],
        compiler_params=pltpu.CompilerParams(collective_id=1, has_side_effects=True),
        name="sum_all",
    )(params)


GX_GY = ("gx_0", "gx_1", "gy")
GX_GY_GZ = GX_GY + ("gz_0", "gz_1")


def local(x, raw, b, c, decay, bias, skip, checkpoints, g):
    raw4, par4 = jnp.tile(raw, (1, 4)), jnp.tile(jnp.stack([bias, decay, skip]), (1, 4))
    term = first(raw4, par4, g, c)
    later, start = exchange(term, checkpoints)
    dx, draw, db, dc, params = second(raw4, par4, x, g, b, c, start, later.reshape(HEADS * WIDTH, STATES))
    sums = sum_all(params)[0]
    return dx, draw, db, dc, sums[:HEADS], sums[HEADS : 2 * HEADS], sums[2 * HEADS : 3 * HEADS]


def solution(mesh):
    torus = Mesh(
        mesh.devices.reshape(4, 2, mesh.shape["gy"], 4, 2), ("gx_0", "gx_1", "gy", "gz_0", "gz_1")
    )
    wide = P(GX_GY_GZ, None)
    return jax.shard_map(
        local,
        mesh=torus,
        in_specs=(wide, wide, wide, wide, P(), P(), P(), P(GX_GY, None, ("gz_0", "gz_1"), None), wide),
        out_specs=(wide, wide, wide, wide, P(), P(), P()),
        check_vma=False,
    )
```

```python
import jax
import jax.numpy as jnp
from jax import lax
from jax.experimental import pallas as pl
from jax.experimental.pallas import tpu as pltpu
from jax.sharding import Mesh
from jax.sharding import PartitionSpec as P

F32, BF16 = jnp.float32, jnp.bfloat16
MESH = pl.DeviceIdType.MESH
HEADS, WIDTH, STATES, SPAN = 32, 64, 128, 256
PART = 4
CHUNK = PART * WIDTH
PIECE = CHUNK // 8


def iota(shape, axis):
    return lax.broadcasted_iota(jnp.int32, shape, axis)


def mm(a, b, ca=1, cb=0):
    return lax.dot_general(a, b, (((ca,), (cb,)), ((), ())), preferred_element_type=F32)


def two(v):
    hi = v.astype(BF16)
    return hi, (v - hi.astype(F32)).astype(BF16)


def three(v):
    hi = v.astype(BF16)
    rest = v - hi.astype(F32)
    mid = rest.astype(BF16)
    return hi, mid, (rest - mid.astype(F32)).astype(BF16)


def lanes(v):
    hi = v.astype(BF16).astype(F32)
    rest = v - hi
    mid = rest.astype(BF16).astype(F32)
    at = iota(v.shape, 1) // HEADS
    return jnp.where(at == 0, hi, jnp.where(at == 1, mid, jnp.where(at == 2, rest - mid, 0.0))).astype(BF16)


def spread_matrix(j):
    row, col = iota((128, CHUNK), 0), iota((128, CHUNK), 1)
    return jnp.where(row % HEADS == col // WIDTH + j * PART, 1.0, 0.0).astype(BF16)


def gather_matrix(j):
    row, col = iota((CHUNK, 128), 0), iota((CHUNK, 128), 1)
    return jnp.where(col % HEADS == row // WIDTH + j * PART, 1.0, 0.0).astype(BF16)


def seg(v, ones):
    a, b, c = three(v)
    return mm(a, ones) + mm(b, ones) + mm(c, ones)


def tri(lower):
    r, c = iota((SPAN, SPAN), 0), iota((SPAN, SPAN), 1)
    return jnp.where((r >= c) if lower else (r <= c), 1.0, 0.0).astype(BF16)


def four(v):
    return jnp.concatenate([v] * 4, axis=1)


def by_head(state, keep):
    return (state.reshape(PART, WIDTH, STATES) * keep[:PART][:, None, :]).reshape(CHUNK, STATES)


class Group:
    def __init__(self, sizes, axes, order=None):
        self.sizes, self.axes = sizes, axes
        self.count = sizes[0] * sizes[1]
        self.at = [lax.axis_index(a) if isinstance(a, str) else lax.axis_index(a[0]) * 2 + lax.axis_index(a[1]) for a in axes]
        self.me = self.at[0] * sizes[1] + self.at[1]
        self.order = order or range(1, self.count)

    def index(self, k, sign):
        m, n = self.sizes
        return (self.at[0] + sign * (k // n) + m) % m, (self.at[1] + sign * (k % n) + n) % n

    def flat(self, k, sign):
        a, b = self.index(k, sign)
        return a * self.sizes[1] + b

    def device(self, k):
        out = {}
        for axis, i in zip(self.axes, self.index(k, 1)):
            if isinstance(axis, str):
                out[axis] = i
            else:
                out[axis[0]], out[axis[1]] = i // 2, i % 2
        return out

    def copy(self, k, src, dst, sems, row):
        return pltpu.make_async_remote_copy(
            src_ref=src, dst_ref=dst, send_sem=sems[0].at[row, k], recv_sem=sems[1].at[row, k],
            device_id=self.device(k), device_id_type=MESH,
        )

    def send(self, src, dst, sems, row):
        copies = []
        for k in self.order:
            copy = self.copy(k, src(self.flat(k, 1)), dst.at[self.me], sems, row)
            copy.start()
            copies.append(copy)
        return copies


def wait_all(copies):
    for copy in copies:
        copy.wait()


def kernel(
    raw_hbm, bias_ref, decay_ref, skip_ref, b_hbm, c_hbm, x_hbm, g_hbm, ckpt_hbm,
    dx_hbm, draw_ref, db_ref, dc_ref, sums_ref,
    raw_ref, b_ref, c_ref, g_v, x_v, dx_v, gh_v, gl_v, z_v, e_ref, f_ref, skip8, small, sh, sl, th, tl, ds_ref, a_acc, r_acc, row_acc,
    term, rec1, inside, lead, tot3, rec3, inside3, lead3, tot4, rec4, out5, rec5, out6, later_v, start_v,
    block, rec_a, rec_b, in_sem, g_sem, x_sem, dx_sem, own_sem, send, recv, send_a, recv_a, send_b, recv_b,
):
    gz = Group((4, 2), ("gz_0", "gz_1"), order=(1, 3, 7, 5, 2, 6, 4))
    gy = Group((8, 1), ("gy", "gz_1"))
    gy.at[1], gy.me, gy.axes = 0, gy.at[0], ("gy",)
    gx = Group((4, 2), ("gx_0", "gx_1"))
    zc = Group((8, 2), (("gx_0", "gz_1"), "gx_1"))
    xy = Group((4, 8), ("gz_0", "gy"))
    sems = (send, recv)

    def columns(j):
        return pl.ds(pl.multiple_of(j * CHUNK, CHUNK), CHUNK)

    barrier = pltpu.get_barrier_semaphore()
    for group in (gz, zc, xy):
        for k in group.order:
            pl.semaphore_signal(barrier, inc=1, device_id=group.device(k), device_id_type=MESH)
    small_in = [
        pltpu.make_async_copy(src, dst, in_sem.at[i])
        for i, (src, dst) in enumerate(((raw_hbm, raw_ref), (c_hbm, c_ref), (b_hbm, b_ref)))
    ]
    g_in = [pltpu.make_async_copy(g_hbm.at[:, columns(j)], g_v.at[j], g_sem.at[j]) for j in range(8)]
    x_in = [pltpu.make_async_copy(x_hbm.at[:, columns(j)], x_v.at[j], x_sem.at[j]) for j in range(8)]
    for copy in small_in + g_in + x_in:
        copy.start()
    small_in[0].wait()

    rows = jnp.concatenate([raw_ref[...]] * 4, axis=0)
    raw = rows.T
    bias, rate = four(bias_ref[...]), jnp.exp(four(decay_ref[...]))
    z = raw + bias
    step = jnp.maximum(z, 0.0) + jnp.log1p(jnp.exp(-jnp.abs(z)))
    low = tri(True)
    q0, q1, q2 = three(step * -rate)
    cum = mm(low, q0) + mm(low, q1) + mm(low, q2)
    e_ref[...] = lanes(jnp.exp(cum))
    back = jnp.exp(-cum)
    f_ref[...] = lanes(back * step)
    small[0], small[1], small[2], small[3] = step, back, back * step, 1.0 / (1.0 + jnp.exp(-z))
    skip8[...] = lanes(jnp.broadcast_to(four(skip_ref[...]), (8, 128)))
    for copy in small_in[1:] + g_in:
        copy.wait()

    def term_step(j, _):
        wide = mm(e_ref[...], spread_matrix(j))
        hi, lo = two(g_v[j].astype(F32) * wide)
        gh_v[j], gl_v[j] = hi, lo
        c = c_ref[...]
        term[j, :CHUNK] = mm(hi, c, 0, 0) + mm(lo, c, 0, 0)
        row, lane = iota((8, 128), 0), iota((8, 128), 1)
        ends = jnp.where(lane % HEADS == row + j * PART, e_ref[SPAN - 1 :, :].astype(F32), 0.0)
        term[j, CHUNK:] = mm(ends.astype(BF16), jnp.ones((128, STATES), BF16))
        return 0

    lax.fori_loop(0, 8, term_step, 0)
    pl.semaphore_wait(barrier, 7 + 15 + 31)
    first_way = gz.send(lambda i: term.at[i], rec1, sems, 0)
    rec1[gz.me] = term[gz.me]

    r, c = iota((SPAN, SPAN), 0), iota((SPAN, SPAN), 1)
    sh[...], sl[...] = two(jnp.where(r >= c, mm(c_ref[...], b_ref[...], 1, 1), 0.0))
    th[...], tl[...] = two(jnp.where(r <= c, mm(b_ref[...], c_ref[...], 1, 1), 0.0))
    for ref in (ds_ref, a_acc, r_acc, row_acc, db_ref, dc_ref):
        ref[...] = jnp.zeros_like(ref)
    for copy in x_in:
        copy.wait()

    def inner_step(j, _):
        f = mm(f_ref[...], spread_matrix(j))
        x = x_v[j].astype(F32)
        xh, xl = two(x * f)
        gh, gl = gh_v[j], gl_v[j]
        y = mm(sh[...], xh) + mm(sl[...], xh) + mm(sh[...], xl)
        z_v[j] = mm(th[...], gh) + mm(tl[...], gh) + mm(th[...], gl)
        ones = gather_matrix(j)
        a_acc[...] += seg((gh.astype(F32) + gl.astype(F32)) * y, ones)
        ds_ref[...] += mm(gh, xh, 1, 1) + mm(gl, xh, 1, 1) + mm(gh, xl, 1, 1)
        direct = jnp.sum(x * g_v[j].astype(F32), axis=0, keepdims=True)
        row_acc[...] += seg(jnp.where(iota((8, CHUNK), 0) == 1, direct, 0.0), ones)
        return 0

    lax.fori_loop(0, 8, inner_step, 0)
    dh, dl = two(jnp.where(r >= c, ds_ref[...], 0.0))
    dc_ref[...] += mm(dh, b_ref[...]) + mm(dl, b_ref[...])
    db_ref[...] += mm(dh, c_ref[...], 0, 0) + mm(dl, c_ref[...], 0, 0)

    wait_all(first_way)
    run = jnp.zeros((CHUNK, STATES), F32)
    keep = jnp.ones((8, STATES), F32)
    for m in reversed(range(8)):
        inside[m] = run
        lead[m] = keep
        own = rec1[m, CHUNK:]
        run = rec1[m, :CHUNK] + by_head(run, own)
        keep = keep * own
    for i in range(8):
        tot3[i, :PIECE] = run[i * PIECE : (i + 1) * PIECE]
        tot3[i, PIECE:] = jnp.broadcast_to(keep[i // 2 : i // 2 + 1], (8, STATES))
    scatter = gy.send(lambda i: tot3.at[i], rec3, sems, 2)
    states = gz.send(lambda i: ckpt_hbm.at[i], start_v, sems, 1)
    own_start = pltpu.make_async_copy(ckpt_hbm.at[gz.me], start_v.at[gz.me], own_sem)
    own_start.start()
    rec3[gy.me] = tot3[gy.me]
    wait_all(scatter)
    run = jnp.zeros((PIECE, STATES), F32)
    keep = jnp.ones((8, STATES), F32)
    for m in reversed(range(8)):
        inside3[m] = run
        lead3[m] = keep
        own = rec3[m, PIECE:]
        run = rec3[m, :PIECE] + run * own[:1]
        keep = keep * own
    tot4[:PIECE] = run
    tot4[PIECE:] = keep
    outer = gx.send(lambda i: tot4, rec4, sems, 3)
    rec4[gx.me] = tot4[...]
    wait_all(outer)
    run = jnp.zeros((PIECE, STATES), F32)
    carry = run
    for m in reversed(range(8)):
        carry = jnp.where(gx.me == m, run, carry)
        run = rec4[m, :PIECE] + run * rec4[m, PIECE : PIECE + 1]
    for m in range(8):
        out5[m] = inside3[m] + lead3[m, :1] * carry
    gather = gy.send(lambda i: out5.at[i], rec5, sems, 4)
    rec5[gy.me] = out5[gy.me]
    wait_all(gather)
    carry = rec5[...].reshape(CHUNK, STATES)
    for m in range(8):
        out6[m] = inside[m] + by_head(carry, lead[m])
    gz.send(lambda i: out6.at[i], later_v, sems, 5)
    later_v[gz.me] = out6[gz.me]

    own_start.wait()
    wait_all(states)

    def chunk_start(j):
        return start_v[:, pl.ds(j * PART, PART)].astype(F32).transpose(1, 0, 2, 3).reshape(CHUNK, STATES)

    def state_step(j, _):
        h = chunk_start(j).astype(BF16)
        gh, gl = gh_v[j], gl_v[j]
        read = mm(c_ref[...], h, 1, 1)
        a_acc[...] += seg((gh.astype(F32) + gl.astype(F32)) * read, gather_matrix(j))
        dc_ref[...] += mm(gh, h) + mm(gl, h)
        return 0

    lax.fori_loop(0, 8, state_step, 0)

    def later_step(j):
        spread, ones = spread_matrix(j), gather_matrix(j)
        f = mm(f_ref[...], spread)
        end = mm(e_ref[SPAN - 16 :, :], spread)[15:, :]
        skip = mm(skip8[...], spread)[:1, :]
        x, g = x_v[j].astype(F32), g_v[j].astype(F32)
        xw = x * f
        later = later_v[j]
        lh, ll = two(later)
        q = (mm(b_ref[...], lh, 1, 1) + mm(b_ref[...], ll, 1, 1)) * end
        zq = z_v[j] + q
        dx_v[j] = (f * zq + skip * g).astype(BF16)
        pltpu.make_async_copy(dx_v.at[j], dx_hbm.at[:, columns(j)], dx_sem.at[j]).start()
        r_acc[...] += seg(x * zq, ones)
        eh, el = two(xw * end)
        db_ref[...] += mm(eh, lh) + mm(el, lh) + mm(eh, ll)
        p0, p1, p2 = three(chunk_start(j) * later)
        one8 = jnp.ones((8, STATES), BF16)
        dots = mm(one8, p0, 1, 1) + mm(one8, p1, 1, 1) + mm(one8, p2, 1, 1)
        at_end = jnp.sum(xw * q, axis=0, keepdims=True) + end * dots
        row_acc[...] += seg(jnp.where(iota((8, CHUNK), 0) == 0, at_end, 0.0), ones)

    def arrive_step(k, _):
        from_k = ORDER(k)
        j = gz.flat(from_k, -1)

        @pl.when(k > 0)
        def _():
            gz.copy(from_k, out6.at[0], later_v.at[0], sems, 5).wait()

        later_step(j)
        return 0

    lax.fori_loop(0, 8, arrive_step, 0)

    last = iota((SPAN, 128), 0) == SPAN - 1
    dcum = a_acc[...] - small[2] * r_acc[...] + jnp.where(last, row_acc[0:1, :], 0.0)
    up = tri(False)
    q0, q1, q2 = three(dcum)
    rc = mm(up, q0) + mm(up, q1) + mm(up, q2)
    rate = jnp.exp(four(decay_ref[...]))
    draw = (small[1] * r_acc[...] - rate * rc) * small[3]
    pd = jnp.sum(rc * small[0], axis=0, keepdims=True) * -rate
    pb = jnp.sum(draw, axis=0, keepdims=True)
    lane = iota((1, 128), 1) // HEADS
    total = jnp.where(lane == 0, pd, jnp.where(lane == 1, pb, jnp.where(lane == 2, row_acc[1:2, :], 0.0)))
    total = jnp.broadcast_to(total, (8, 128))
    block[0] = total
    near = zc.send(lambda i: block.at[0], rec_a, (send_a, recv_a), 0)
    rec_a[zc.me] = total
    draw_ref[...] = draw.T[:HEADS, :]
    wait_all(near)
    total = jnp.sum(rec_a[...], axis=0)
    block[1] = total
    far = xy.send(lambda i: block.at[1], rec_b, (send_b, recv_b), 0)
    rec_b[xy.me] = total
    for j in range(8):
        pltpu.make_async_copy(dx_v.at[j], dx_hbm.at[:, columns(j)], dx_sem.at[j]).wait()
    wait_all(far)
    sums_ref[...] = jnp.sum(rec_b[...], axis=0)


def ORDER(k):
    return (k % 4) * 2 + k // 4


def local(x, raw, b, c, decay, bias, skip, checkpoints, g):
    vmem, hbm = pl.BlockSpec(memory_space=pltpu.VMEM), pl.BlockSpec(memory_space=pltpu.HBM)
    buf = lambda *shape: pltpu.VMEM(shape, F32)
    half = lambda *shape: pltpu.VMEM(shape, BF16)
    dma = lambda *shape: pltpu.SemaphoreType.DMA(shape)
    row = lambda v: v.reshape(1, HEADS)
    dx, draw, db, dc, sums = pl.pallas_call(
        kernel,
        out_shape=(
            jax.ShapeDtypeStruct((SPAN, HEADS * WIDTH), BF16),
            jax.ShapeDtypeStruct((HEADS, SPAN), F32),
            jax.ShapeDtypeStruct((SPAN, STATES), F32),
            jax.ShapeDtypeStruct((SPAN, STATES), F32),
            jax.ShapeDtypeStruct((8, 128), F32),
        ),
        in_specs=[hbm, vmem, vmem, vmem, hbm, hbm, hbm, hbm, hbm],
        out_specs=(hbm, vmem, vmem, vmem, vmem),
        scratch_shapes=[
            buf(HEADS, SPAN), half(SPAN, STATES), half(SPAN, STATES),
            half(8, SPAN, CHUNK), half(8, SPAN, CHUNK), half(8, SPAN, CHUNK), half(8, SPAN, CHUNK),
            half(8, SPAN, CHUNK), buf(8, SPAN, CHUNK), half(SPAN, 128), half(SPAN, 128), half(8, 128),
            buf(4, SPAN, 128), half(SPAN, SPAN), half(SPAN, SPAN), half(SPAN, SPAN), half(SPAN, SPAN),
            buf(SPAN, SPAN), buf(SPAN, 128), buf(SPAN, 128), buf(8, 128),
            buf(8, CHUNK + 8, STATES), buf(8, CHUNK + 8, STATES), buf(8, CHUNK, STATES), buf(8, 8, STATES),
            buf(8, PIECE + 8, STATES), buf(8, PIECE + 8, STATES), buf(8, PIECE, STATES), buf(8, 8, STATES),
            buf(PIECE + 8, STATES), buf(8, PIECE + 8, STATES), buf(8, PIECE, STATES), buf(8, PIECE, STATES),
            buf(8, CHUNK, STATES), buf(8, CHUNK, STATES), half(8, HEADS, 8, STATES),
            buf(2, 8, 128), buf(16, 8, 128), buf(32, 8, 128),
            dma(3), dma(8), dma(8), dma(8), pltpu.SemaphoreType.DMA, dma(6, 8), dma(6, 8),
            dma(1, 16), dma(1, 16), dma(1, 32), dma(1, 32),
        ],
        compiler_params=pltpu.CompilerParams(collective_id=0, has_side_effects=True, vmem_limit_bytes=67_000_000),
        name="spans",
    )(raw.T, row(bias), row(decay), row(skip), b, c, x, g, checkpoints)
    sums = sums[0]
    return dx, draw.T, db, dc, sums[:HEADS], sums[HEADS : 2 * HEADS], sums[2 * HEADS : 3 * HEADS]


GX_GY_GZ = ("gx_0", "gx_1", "gy", "gz_0", "gz_1")


def solution(mesh):
    torus = Mesh(mesh.devices.reshape(4, 2, mesh.shape["gy"], 4, 2), GX_GY_GZ)
    wide = P(GX_GY_GZ, None)
    return jax.shard_map(
        local,
        mesh=torus,
        in_specs=(wide, wide, wide, wide, P(), P(), P(), P(GX_GY_GZ[:3], None, GX_GY_GZ[3:], None), wide),
        out_specs=(wide, wide, wide, wide, P(), P(), P()),
        check_vma=False,
    )
```

```python
import jax
import jax.numpy as jnp
from jax import lax
from jax.experimental import pallas as pl
from jax.experimental.pallas import tpu as pltpu
from jax.sharding import Mesh
from jax.sharding import PartitionSpec as P

F32, BF16 = jnp.float32, jnp.bfloat16
MESH = pl.DeviceIdType.MESH
HEADS, WIDTH, STATES, SPAN = 32, 64, 128, 256
PART = 4
CHUNK = PART * WIDTH
PIECE = CHUNK // 8


def iota(shape, axis):
    return lax.broadcasted_iota(jnp.int32, shape, axis)


def mm(a, b, ca=1, cb=0):
    return lax.dot_general(a, b, (((ca,), (cb,)), ((), ())), preferred_element_type=F32)


def two(v):
    hi = v.astype(BF16)
    return hi, (v - hi.astype(F32)).astype(BF16)


def three(v):
    hi = v.astype(BF16)
    rest = v - hi.astype(F32)
    mid = rest.astype(BF16)
    return hi, mid, (rest - mid.astype(F32)).astype(BF16)


def lanes(v):
    hi = v.astype(BF16).astype(F32)
    rest = v - hi
    mid = rest.astype(BF16).astype(F32)
    at = iota(v.shape, 1) // HEADS
    return jnp.where(at == 0, hi, jnp.where(at == 1, mid, jnp.where(at == 2, rest - mid, 0.0))).astype(BF16)


def spread_matrix(j):
    row, col = iota((128, CHUNK), 0), iota((128, CHUNK), 1)
    return jnp.where(row % HEADS == col // WIDTH + j * PART, 1.0, 0.0).astype(BF16)


def gather_matrix(j):
    row, col = iota((CHUNK, 128), 0), iota((CHUNK, 128), 1)
    return jnp.where(col % HEADS == row // WIDTH + j * PART, 1.0, 0.0).astype(BF16)


def seg(v, ones):
    a, b, c = three(v)
    return mm(a, ones) + mm(b, ones) + mm(c, ones)


def tri(lower):
    r, c = iota((SPAN, SPAN), 0), iota((SPAN, SPAN), 1)
    return jnp.where((r >= c) if lower else (r <= c), 1.0, 0.0).astype(BF16)


def four(v):
    return jnp.concatenate([v] * 4, axis=1)


def by_head(state, keep):
    return (state.reshape(PART, WIDTH, STATES) * keep[:PART][:, None, :]).reshape(CHUNK, STATES)


class Group:
    def __init__(self, sizes, axes, order=None):
        self.sizes, self.axes = sizes, axes
        self.count = sizes[0] * sizes[1]
        self.at = [lax.axis_index(a) if isinstance(a, str) else lax.axis_index(a[0]) * 2 + lax.axis_index(a[1]) for a in axes]
        self.me = self.at[0] * sizes[1] + self.at[1]
        self.order = order or range(1, self.count)

    def index(self, k, sign):
        m, n = self.sizes
        return (self.at[0] + sign * (k // n) + m) % m, (self.at[1] + sign * (k % n) + n) % n

    def flat(self, k, sign):
        a, b = self.index(k, sign)
        return a * self.sizes[1] + b

    def device(self, k):
        out = {}
        for axis, i in zip(self.axes, self.index(k, 1)):
            if isinstance(axis, str):
                out[axis] = i
            else:
                out[axis[0]], out[axis[1]] = i // 2, i % 2
        return out

    def copy(self, k, src, dst, sems, row):
        return pltpu.make_async_remote_copy(
            src_ref=src, dst_ref=dst, send_sem=sems[0].at[row, k], recv_sem=sems[1].at[row, k],
            device_id=self.device(k), device_id_type=MESH,
        )

    def send(self, src, dst, sems, row):
        copies = []
        for k in self.order:
            copy = self.copy(k, src(self.flat(k, 1)), dst.at[self.me], sems, row)
            copy.start()
            copies.append(copy)
        return copies


def wait_all(copies):
    for copy in copies:
        copy.wait()


def kernel(
    raw_hbm, bias_ref, decay_ref, skip_ref, b_hbm, c_hbm, x_hbm, g_hbm, ckpt_hbm,
    dx_hbm, draw_ref, db_ref, dc_ref, sums_ref,
    raw_ref, b_ref, c_ref, g_v, x_v, dx_v, gh_v, gl_v, z_v, e_ref, f_ref, skip8, small, sh, sl, th, tl, ds_ref, a_acc, r_acc, row_acc,
    term, rec1, inside, lead, tot3, rec3, inside3, lead3, tot4, rec4, out5, rec5, out6, later_v, start_v,
    block, rec_a, rec_b, in_sem, g_sem, x_sem, dx_sem, own_sem, send, recv, send_a, recv_a, send_b, recv_b,
):
    gz = Group((4, 2), ("gz_0", "gz_1"), order=(1, 3, 7, 5, 2, 6, 4))
    gy = Group((8, 1), ("gy", "gz_1"))
    gy.at[1], gy.me, gy.axes = 0, gy.at[0], ("gy",)
    gx = Group((4, 2), ("gx_0", "gx_1"))
    zc = Group((8, 2), (("gx_0", "gz_1"), "gx_1"))
    xy = Group((4, 8), ("gz_0", "gy"))
    sems = (send, recv)

    def columns(j):
        return pl.ds(pl.multiple_of(j * CHUNK, CHUNK), CHUNK)

    small_in = [
        pltpu.make_async_copy(src, dst, in_sem.at[i])
        for i, (src, dst) in enumerate(((raw_hbm, raw_ref), (c_hbm, c_ref), (b_hbm, b_ref)))
    ]
    g_in = [pltpu.make_async_copy(g_hbm.at[:, columns(j)], g_v.at[j], g_sem.at[j]) for j in range(8)]
    x_in = [pltpu.make_async_copy(x_hbm.at[:, columns(j)], x_v.at[j], x_sem.at[j]) for j in range(8)]
    for copy in small_in + g_in:
        copy.start()
    barrier = pltpu.get_barrier_semaphore()
    for group in (gz, zc, xy):
        for k in group.order:
            pl.semaphore_signal(barrier, inc=1, device_id=group.device(k), device_id_type=MESH)
    for copy in x_in:
        copy.start()
    small_in[0].wait()

    rows = jnp.concatenate([raw_ref[...]] * 4, axis=0)
    raw = rows.T
    bias, rate = four(bias_ref[...]), jnp.exp(four(decay_ref[...]))
    z = raw + bias
    step = jnp.maximum(z, 0.0) + jnp.log1p(jnp.exp(-jnp.abs(z)))
    low = tri(True)
    q0, q1, q2 = three(step * -rate)
    cum = mm(low, q0) + mm(low, q1) + mm(low, q2)
    e_ref[...] = lanes(jnp.exp(cum))
    back = jnp.exp(-cum)
    f_ref[...] = lanes(back * step)
    small[0], small[1], small[2], small[3] = step, back, back * step, 1.0 / (1.0 + jnp.exp(-z))
    skip8[...] = lanes(jnp.broadcast_to(four(skip_ref[...]), (8, 128)))
    for copy in small_in[1:] + g_in:
        copy.wait()

    def term_step(j, _):
        wide = mm(e_ref[...], spread_matrix(j))
        hi, lo = two(g_v[j].astype(F32) * wide)
        gh_v[j], gl_v[j] = hi, lo
        c = c_ref[...]
        term[j, :CHUNK] = mm(hi, c, 0, 0) + mm(lo, c, 0, 0)
        row, lane = iota((8, 128), 0), iota((8, 128), 1)
        ends = jnp.where(lane % HEADS == row + j * PART, e_ref[SPAN - 1 :, :].astype(F32), 0.0)
        term[j, CHUNK:] = mm(ends.astype(BF16), jnp.ones((128, STATES), BF16))
        return 0

    lax.fori_loop(0, 8, term_step, 0)
    pl.semaphore_wait(barrier, 7 + 15 + 31)
    first_way = gz.send(lambda i: term.at[i], rec1, sems, 0)
    rec1[gz.me] = term[gz.me]

    r, c = iota((SPAN, SPAN), 0), iota((SPAN, SPAN), 1)
    sh[...], sl[...] = two(jnp.where(r >= c, mm(c_ref[...], b_ref[...], 1, 1), 0.0))
    th[...], tl[...] = two(jnp.where(r <= c, mm(b_ref[...], c_ref[...], 1, 1), 0.0))
    for ref in (ds_ref, a_acc, r_acc, row_acc, db_ref, dc_ref):
        ref[...] = jnp.zeros_like(ref)
    for copy in x_in:
        copy.wait()

    def inner_step(j, _):
        f = mm(f_ref[...], spread_matrix(j))
        x = x_v[j].astype(F32)
        xh, xl = two(x * f)
        gh, gl = gh_v[j], gl_v[j]
        y = mm(sh[...], xh) + mm(sl[...], xh) + mm(sh[...], xl)
        z_v[j] = mm(th[...], gh) + mm(tl[...], gh) + mm(th[...], gl)
        ones = gather_matrix(j)
        a_acc[...] += seg((gh.astype(F32) + gl.astype(F32)) * y, ones)
        ds_ref[...] += mm(gh, xh, 1, 1) + mm(gl, xh, 1, 1) + mm(gh, xl, 1, 1)
        direct = jnp.sum(x * g_v[j].astype(F32), axis=0, keepdims=True)
        row_acc[...] += seg(jnp.where(iota((8, CHUNK), 0) == 1, direct, 0.0), ones)
        return 0

    lax.fori_loop(0, 8, inner_step, 0)
    dh, dl = two(jnp.where(r >= c, ds_ref[...], 0.0))
    dc_ref[...] += mm(dh, b_ref[...]) + mm(dl, b_ref[...])
    db_ref[...] += mm(dh, c_ref[...], 0, 0) + mm(dl, c_ref[...], 0, 0)

    wait_all(first_way)
    run = jnp.zeros((CHUNK, STATES), F32)
    keep = jnp.ones((8, STATES), F32)
    for m in reversed(range(8)):
        inside[m] = run
        lead[m] = keep
        own = rec1[m, CHUNK:]
        run = rec1[m, :CHUNK] + by_head(run, own)
        keep = keep * own
    for i in range(8):
        tot3[i, :PIECE] = run[i * PIECE : (i + 1) * PIECE]
        tot3[i, PIECE:] = jnp.broadcast_to(keep[i // 2 : i // 2 + 1], (8, STATES))
    scatter = gy.send(lambda i: tot3.at[i], rec3, sems, 2)
    states = gz.send(lambda i: ckpt_hbm.at[i], start_v, sems, 1)
    own_start = pltpu.make_async_copy(ckpt_hbm.at[gz.me], start_v.at[gz.me], own_sem)
    own_start.start()
    rec3[gy.me] = tot3[gy.me]
    wait_all(scatter)
    run = jnp.zeros((PIECE, STATES), F32)
    keep = jnp.ones((8, STATES), F32)
    for m in reversed(range(8)):
        inside3[m] = run
        lead3[m] = keep
        own = rec3[m, PIECE:]
        run = rec3[m, :PIECE] + run * own[:1]
        keep = keep * own
    tot4[:PIECE] = run
    tot4[PIECE:] = keep
    outer = gx.send(lambda i: tot4, rec4, sems, 3)
    rec4[gx.me] = tot4[...]
    wait_all(outer)
    run = jnp.zeros((PIECE, STATES), F32)
    carry = run
    for m in reversed(range(8)):
        carry = jnp.where(gx.me == m, run, carry)
        run = rec4[m, :PIECE] + run * rec4[m, PIECE : PIECE + 1]
    for m in range(8):
        out5[m] = inside3[m] + lead3[m, :1] * carry
    gather = gy.send(lambda i: out5.at[i], rec5, sems, 4)
    rec5[gy.me] = out5[gy.me]
    wait_all(gather)
    carry = rec5[...].reshape(CHUNK, STATES)
    for m in range(8):
        out6[m] = inside[m] + by_head(carry, lead[m])
    gz.send(lambda i: out6.at[i], later_v, sems, 5)
    later_v[gz.me] = out6[gz.me]

    own_start.wait()
    wait_all(states)

    def chunk_start(j):
        return start_v[:, pl.ds(j * PART, PART)].astype(F32).transpose(1, 0, 2, 3).reshape(CHUNK, STATES)

    def state_step(j, _):
        h = chunk_start(j).astype(BF16)
        gh, gl = gh_v[j], gl_v[j]
        read = mm(c_ref[...], h, 1, 1)
        a_acc[...] += seg((gh.astype(F32) + gl.astype(F32)) * read, gather_matrix(j))
        dc_ref[...] += mm(gh, h) + mm(gl, h)
        return 0

    lax.fori_loop(0, 8, state_step, 0)

    def later_step(j):
        spread, ones = spread_matrix(j), gather_matrix(j)
        f = mm(f_ref[...], spread)
        end = mm(e_ref[SPAN - 16 :, :], spread)[15:, :]
        skip = mm(skip8[...], spread)[:1, :]
        x, g = x_v[j].astype(F32), g_v[j].astype(F32)
        xw = x * f
        later = later_v[j]
        lh, ll = two(later)
        q = (mm(b_ref[...], lh, 1, 1) + mm(b_ref[...], ll, 1, 1)) * end
        zq = z_v[j] + q
        dx_v[j] = (f * zq + skip * g).astype(BF16)
        pltpu.make_async_copy(dx_v.at[j], dx_hbm.at[:, columns(j)], dx_sem.at[j]).start()
        r_acc[...] += seg(x * zq, ones)
        eh, el = two(xw * end)
        db_ref[...] += mm(eh, lh) + mm(el, lh) + mm(eh, ll)
        p0, p1, p2 = three(chunk_start(j) * later)
        one8 = jnp.ones((8, STATES), BF16)
        dots = mm(one8, p0, 1, 1) + mm(one8, p1, 1, 1) + mm(one8, p2, 1, 1)
        at_end = jnp.sum(xw * q, axis=0, keepdims=True) + end * dots
        row_acc[...] += seg(jnp.where(iota((8, CHUNK), 0) == 0, at_end, 0.0), ones)

    def arrive_step(k, _):
        from_k = ORDER(k)
        j = gz.flat(from_k, -1)

        @pl.when(k > 0)
        def _():
            gz.copy(from_k, out6.at[0], later_v.at[0], sems, 5).wait()

        later_step(j)
        return 0

    lax.fori_loop(0, 8, arrive_step, 0)

    last = iota((SPAN, 128), 0) == SPAN - 1
    dcum = a_acc[...] - small[2] * r_acc[...] + jnp.where(last, row_acc[0:1, :], 0.0)
    up = tri(False)
    q0, q1, q2 = three(dcum)
    rc = mm(up, q0) + mm(up, q1) + mm(up, q2)
    rate = jnp.exp(four(decay_ref[...]))
    draw = (small[1] * r_acc[...] - rate * rc) * small[3]
    pd = jnp.sum(rc * small[0], axis=0, keepdims=True) * -rate
    pb = jnp.sum(draw, axis=0, keepdims=True)
    lane = iota((1, 128), 1) // HEADS
    total = jnp.where(lane == 0, pd, jnp.where(lane == 1, pb, jnp.where(lane == 2, row_acc[1:2, :], 0.0)))
    total = jnp.broadcast_to(total, (8, 128))
    block[0] = total
    near = zc.send(lambda i: block.at[0], rec_a, (send_a, recv_a), 0)
    rec_a[zc.me] = total
    draw_ref[...] = draw.T[:HEADS, :]
    wait_all(near)
    total = jnp.sum(rec_a[...], axis=0)
    block[1] = total
    far = xy.send(lambda i: block.at[1], rec_b, (send_b, recv_b), 0)
    rec_b[xy.me] = total
    for j in range(8):
        pltpu.make_async_copy(dx_v.at[j], dx_hbm.at[:, columns(j)], dx_sem.at[j]).wait()
    wait_all(far)
    sums_ref[...] = jnp.sum(rec_b[...], axis=0)


def ORDER(k):
    return (k % 4) * 2 + k // 4


def local(x, raw, b, c, decay, bias, skip, checkpoints, g):
    vmem, hbm = pl.BlockSpec(memory_space=pltpu.VMEM), pl.BlockSpec(memory_space=pltpu.HBM)
    buf = lambda *shape: pltpu.VMEM(shape, F32)
    half = lambda *shape: pltpu.VMEM(shape, BF16)
    dma = lambda *shape: pltpu.SemaphoreType.DMA(shape)
    row = lambda v: v.reshape(1, HEADS)
    keep = lambda v: pltpu.with_memory_space_constraint(v, pltpu.HBM)
    dx, draw, db, dc, sums = pl.pallas_call(
        kernel,
        out_shape=(
            jax.ShapeDtypeStruct((SPAN, HEADS * WIDTH), BF16),
            jax.ShapeDtypeStruct((HEADS, SPAN), F32),
            jax.ShapeDtypeStruct((SPAN, STATES), F32),
            jax.ShapeDtypeStruct((SPAN, STATES), F32),
            jax.ShapeDtypeStruct((8, 128), F32),
        ),
        in_specs=[hbm, vmem, vmem, vmem, hbm, hbm, hbm, hbm, hbm],
        out_specs=(hbm, vmem, vmem, vmem, vmem),
        scratch_shapes=[
            buf(HEADS, SPAN), half(SPAN, STATES), half(SPAN, STATES),
            half(8, SPAN, CHUNK), half(8, SPAN, CHUNK), half(8, SPAN, CHUNK), half(8, SPAN, CHUNK),
            half(8, SPAN, CHUNK), buf(8, SPAN, CHUNK), half(SPAN, 128), half(SPAN, 128), half(8, 128),
            buf(4, SPAN, 128), half(SPAN, SPAN), half(SPAN, SPAN), half(SPAN, SPAN), half(SPAN, SPAN),
            buf(SPAN, SPAN), buf(SPAN, 128), buf(SPAN, 128), buf(8, 128),
            buf(8, CHUNK + 8, STATES), buf(8, CHUNK + 8, STATES), buf(8, CHUNK, STATES), buf(8, 8, STATES),
            buf(8, PIECE + 8, STATES), buf(8, PIECE + 8, STATES), buf(8, PIECE, STATES), buf(8, 8, STATES),
            buf(PIECE + 8, STATES), buf(8, PIECE + 8, STATES), buf(8, PIECE, STATES), buf(8, PIECE, STATES),
            buf(8, CHUNK, STATES), buf(8, CHUNK, STATES), half(8, HEADS, 8, STATES),
            buf(2, 8, 128), buf(16, 8, 128), buf(32, 8, 128),
            dma(3), dma(8), dma(8), dma(8), pltpu.SemaphoreType.DMA, dma(6, 8), dma(6, 8),
            dma(1, 16), dma(1, 16), dma(1, 32), dma(1, 32),
        ],
        compiler_params=pltpu.CompilerParams(collective_id=0, has_side_effects=True, vmem_limit_bytes=40 * 2**20),
        name="spans",
    )(keep(raw.T), row(bias), row(decay), row(skip), keep(b), keep(c), keep(x), keep(g), keep(checkpoints))
    sums = sums[0]
    return dx, draw.T, db, dc, sums[:HEADS], sums[HEADS : 2 * HEADS], sums[2 * HEADS : 3 * HEADS]


GX_GY_GZ = ("gx_0", "gx_1", "gy", "gz_0", "gz_1")


def solution(mesh):
    torus = Mesh(mesh.devices.reshape(4, 2, mesh.shape["gy"], 4, 2), GX_GY_GZ)
    wide = P(GX_GY_GZ, None)
    return jax.shard_map(
        local,
        mesh=torus,
        in_specs=(wide, wide, wide, wide, P(), P(), P(), P(GX_GY_GZ[:3], None, GX_GY_GZ[3:], None), wide),
        out_specs=(wide, wide, wide, wide, P(), P(), P()),
        check_vma=False,
    )
```

```python
import jax
import jax.numpy as jnp
from jax import lax
from jax.experimental import pallas as pl
from jax.experimental.pallas import tpu as pltpu
from jax.sharding import Mesh
from jax.sharding import PartitionSpec as P

F32, BF16 = jnp.float32, jnp.bfloat16
MESH = pl.DeviceIdType.MESH
HEADS, WIDTH, STATES, SPAN = 32, 64, 128, 256
PART = 4
CHUNK = PART * WIDTH
PIECE = CHUNK // 8


def iota(shape, axis):
    return lax.broadcasted_iota(jnp.int32, shape, axis)


def mm(a, b, ca=1, cb=0):
    return lax.dot_general(a, b, (((ca,), (cb,)), ((), ())), preferred_element_type=F32)


def two(v):
    hi = v.astype(BF16)
    return hi, (v - hi.astype(F32)).astype(BF16)


def three(v):
    hi = v.astype(BF16)
    rest = v - hi.astype(F32)
    mid = rest.astype(BF16)
    return hi, mid, (rest - mid.astype(F32)).astype(BF16)


def lanes(v):
    hi = v.astype(BF16).astype(F32)
    rest = v - hi
    mid = rest.astype(BF16).astype(F32)
    at = iota(v.shape, 1) // HEADS
    return jnp.where(at == 0, hi, jnp.where(at == 1, mid, jnp.where(at == 2, rest - mid, 0.0))).astype(BF16)


def spread_matrix(j):
    row, col = iota((128, CHUNK), 0), iota((128, CHUNK), 1)
    return jnp.where(row % HEADS == col // WIDTH + j * PART, 1.0, 0.0).astype(BF16)


def gather_matrix(j):
    row, col = iota((CHUNK, 128), 0), iota((CHUNK, 128), 1)
    return jnp.where(col % HEADS == row // WIDTH + j * PART, 1.0, 0.0).astype(BF16)


def seg(v, ones):
    a, b, c = three(v)
    return mm(a, ones) + mm(b, ones) + mm(c, ones)


def tri(lower):
    r, c = iota((SPAN, SPAN), 0), iota((SPAN, SPAN), 1)
    return jnp.where((r >= c) if lower else (r <= c), 1.0, 0.0).astype(BF16)


def four(v):
    return jnp.concatenate([v] * 4, axis=1)


def by_head(state, keep):
    return (state.reshape(PART, WIDTH, STATES) * keep[:PART][:, None, :]).reshape(CHUNK, STATES)


class Group:
    def __init__(self, sizes, axes, order=None):
        self.sizes, self.axes = sizes, axes
        self.count = sizes[0] * sizes[1]
        self.at = [lax.axis_index(a) if isinstance(a, str) else lax.axis_index(a[0]) * 2 + lax.axis_index(a[1]) for a in axes]
        self.me = self.at[0] * sizes[1] + self.at[1]
        self.order = order or range(1, self.count)

    def index(self, k, sign):
        m, n = self.sizes
        return (self.at[0] + sign * (k // n) + m) % m, (self.at[1] + sign * (k % n) + n) % n

    def flat(self, k, sign):
        a, b = self.index(k, sign)
        return a * self.sizes[1] + b

    def device(self, k):
        out = {}
        for axis, i in zip(self.axes, self.index(k, 1)):
            if isinstance(axis, str):
                out[axis] = i
            else:
                out[axis[0]], out[axis[1]] = i // 2, i % 2
        return out

    def copy(self, k, src, dst, sems, row):
        return pltpu.make_async_remote_copy(
            src_ref=src, dst_ref=dst, send_sem=sems[0].at[row, k], recv_sem=sems[1].at[row, k],
            device_id=self.device(k), device_id_type=MESH,
        )

    def send(self, src, dst, sems, row):
        copies = []
        for k in self.order:
            copy = self.copy(k, src(self.flat(k, 1)), dst.at[self.me], sems, row)
            copy.start()
            copies.append(copy)
        return copies


def wait_all(copies):
    for copy in copies:
        copy.wait()


def kernel(
    raw_hbm, bias_ref, decay_ref, skip_ref, b_hbm, c_hbm, x_hbm, g_hbm, ckpt_hbm,
    dx_hbm, draw_ref, db_ref, dc_ref, sums_ref,
    raw_ref, b_ref, c_ref, g_v, x_v, dx_v, gh_v, gl_v, z_v, e_ref, f_ref, skip8, small, sh, sl, th, tl, ds_ref, a_acc, r_acc, row_acc,
    term, rec1, inside, lead, tot3, rec3, inside3, lead3, tot4, rec4, out5, rec5, out6, later_v, start_v,
    block, rec_a, rec_b, in_sem, g_sem, x_sem, dx_sem, own_sem, send, recv, send_a, recv_a, send_b, recv_b,
):
    gz = Group((4, 2), ("gz_0", "gz_1"), order=(1, 3, 7, 5, 2, 6, 4))
    gy = Group((8, 1), ("gy", "gz_1"))
    gy.at[1], gy.me, gy.axes = 0, gy.at[0], ("gy",)
    gx = Group((4, 2), ("gx_0", "gx_1"))
    zc = Group((8, 2), (("gx_0", "gz_1"), "gx_1"))
    xy = Group((4, 8), ("gz_0", "gy"))
    sems = (send, recv)

    def columns(j):
        return pl.ds(pl.multiple_of(j * CHUNK, CHUNK), CHUNK)

    small_in = [
        pltpu.make_async_copy(src, dst, in_sem.at[i])
        for i, (src, dst) in enumerate(((raw_hbm, raw_ref), (c_hbm, c_ref), (b_hbm, b_ref)))
    ]
    g_in = [pltpu.make_async_copy(g_hbm.at[:, columns(j)], g_v.at[j], g_sem.at[j]) for j in range(8)]
    x_in = [pltpu.make_async_copy(x_hbm.at[:, columns(j)], x_v.at[j], x_sem.at[j]) for j in range(8)]
    for copy in small_in + g_in:
        copy.start()
    barrier = pltpu.get_barrier_semaphore()
    for group in (gz, zc, xy):
        for k in group.order:
            pl.semaphore_signal(barrier, inc=1, device_id=group.device(k), device_id_type=MESH)
    for copy in x_in:
        copy.start()
    small_in[0].wait()

    rows = jnp.concatenate([raw_ref[...]] * 4, axis=0)
    raw = rows.T
    bias, rate = four(bias_ref[...]), jnp.exp(four(decay_ref[...]))
    z = raw + bias
    step = jnp.maximum(z, 0.0) + jnp.log1p(jnp.exp(-jnp.abs(z)))
    low = tri(True)
    q0, q1, q2 = three(step * -rate)
    cum = mm(low, q0) + mm(low, q1) + mm(low, q2)
    e_ref[...] = lanes(jnp.exp(cum))
    back = jnp.exp(-cum)
    f_ref[...] = lanes(back * step)
    small[0], small[1], small[2], small[3] = step, back, back * step, 1.0 / (1.0 + jnp.exp(-z))
    skip8[...] = lanes(jnp.broadcast_to(four(skip_ref[...]), (8, 128)))
    for copy in small_in[1:] + g_in:
        copy.wait()

    def term_step(j, _):
        wide = mm(e_ref[...], spread_matrix(j))
        hi, lo = two(g_v[j].astype(F32) * wide)
        gh_v[j], gl_v[j] = hi, lo
        c = c_ref[...]
        term[j, :CHUNK] = mm(hi, c, 0, 0) + mm(lo, c, 0, 0)
        row, lane = iota((8, 128), 0), iota((8, 128), 1)
        ends = jnp.where(lane % HEADS == row + j * PART, e_ref[SPAN - 1 :, :].astype(F32), 0.0)
        term[j, CHUNK:] = mm(ends.astype(BF16), jnp.ones((128, STATES), BF16))
        return 0

    lax.fori_loop(0, 8, term_step, 0)
    pl.semaphore_wait(barrier, 7 + 15 + 31)
    first_way = gz.send(lambda i: term.at[i], rec1, sems, 0)
    rec1[gz.me] = term[gz.me]

    r, c = iota((SPAN, SPAN), 0), iota((SPAN, SPAN), 1)
    sh[...], sl[...] = two(jnp.where(r >= c, mm(c_ref[...], b_ref[...], 1, 1), 0.0))
    th[...], tl[...] = two(jnp.where(r <= c, mm(b_ref[...], c_ref[...], 1, 1), 0.0))
    for ref in (ds_ref, a_acc, r_acc, row_acc, db_ref, dc_ref):
        ref[...] = jnp.zeros_like(ref)
    for copy in x_in:
        copy.wait()

    def inner_step(j, _):
        f = mm(f_ref[...], spread_matrix(j))
        x = x_v[j].astype(F32)
        xh, xl = two(x * f)
        gh, gl = gh_v[j], gl_v[j]
        y = mm(sh[...], xh) + mm(sl[...], xh) + mm(sh[...], xl)
        z_v[j] = mm(th[...], gh) + mm(tl[...], gh) + mm(th[...], gl)
        ones = gather_matrix(j)
        a_acc[...] += seg((gh.astype(F32) + gl.astype(F32)) * y, ones)
        ds_ref[...] += mm(gh, xh, 1, 1) + mm(gl, xh, 1, 1) + mm(gh, xl, 1, 1)
        direct = jnp.sum(x * g_v[j].astype(F32), axis=0, keepdims=True)
        row_acc[...] += seg(jnp.where(iota((8, CHUNK), 0) == 1, direct, 0.0), ones)
        return 0

    lax.fori_loop(0, 8, inner_step, 0)
    dh, dl = two(jnp.where(r >= c, ds_ref[...], 0.0))
    dc_ref[...] += mm(dh, b_ref[...]) + mm(dl, b_ref[...])
    db_ref[...] += mm(dh, c_ref[...], 0, 0) + mm(dl, c_ref[...], 0, 0)

    wait_all(first_way)
    run = jnp.zeros((CHUNK, STATES), F32)
    keep = jnp.ones((8, STATES), F32)
    for m in reversed(range(8)):
        inside[m] = run
        lead[m] = keep
        own = rec1[m, CHUNK:]
        run = rec1[m, :CHUNK] + by_head(run, own)
        keep = keep * own
    for i in range(8):
        tot3[i, :PIECE] = run[i * PIECE : (i + 1) * PIECE]
        tot3[i, PIECE:] = jnp.broadcast_to(keep[i // 2 : i // 2 + 1], (8, STATES))
    scatter = gy.send(lambda i: tot3.at[i], rec3, sems, 2)
    states = gz.send(lambda i: ckpt_hbm.at[i], start_v, sems, 1)
    own_start = pltpu.make_async_copy(ckpt_hbm.at[gz.me], start_v.at[gz.me], own_sem)
    own_start.start()
    rec3[gy.me] = tot3[gy.me]
    wait_all(scatter)
    run = jnp.zeros((PIECE, STATES), F32)
    keep = jnp.ones((8, STATES), F32)
    for m in reversed(range(8)):
        inside3[m] = run
        lead3[m] = keep
        own = rec3[m, PIECE:]
        run = rec3[m, :PIECE] + run * own[:1]
        keep = keep * own
    tot4[:PIECE] = run
    tot4[PIECE:] = keep
    outer = gx.send(lambda i: tot4, rec4, sems, 3)
    rec4[gx.me] = tot4[...]
    wait_all(outer)
    run = jnp.zeros((PIECE, STATES), F32)
    carry = run
    for m in reversed(range(8)):
        carry = jnp.where(gx.me == m, run, carry)
        run = rec4[m, :PIECE] + run * rec4[m, PIECE : PIECE + 1]
    for m in range(8):
        out5[m] = inside3[m] + lead3[m, :1] * carry
    gather = gy.send(lambda i: out5.at[i], rec5, sems, 4)
    rec5[gy.me] = out5[gy.me]
    wait_all(gather)
    carry = rec5[...].reshape(CHUNK, STATES)
    for m in range(8):
        out6[m] = inside[m] + by_head(carry, lead[m])
    gz.send(lambda i: out6.at[i], later_v, sems, 5)
    later_v[gz.me] = out6[gz.me]

    own_start.wait()
    wait_all(states)

    def chunk_start(j):
        return start_v[:, pl.ds(j * PART, PART)].astype(F32).transpose(1, 0, 2, 3).reshape(CHUNK, STATES)

    def state_step(j, _):
        h = chunk_start(j).astype(BF16)
        gh, gl = gh_v[j], gl_v[j]
        read = mm(c_ref[...], h, 1, 1)
        a_acc[...] += seg((gh.astype(F32) + gl.astype(F32)) * read, gather_matrix(j))
        dc_ref[...] += mm(gh, h) + mm(gl, h)
        return 0

    lax.fori_loop(0, 8, state_step, 0)

    def later_step(j):
        spread, ones = spread_matrix(j), gather_matrix(j)
        f = mm(f_ref[...], spread)
        end = mm(e_ref[SPAN - 16 :, :], spread)[15:, :]
        skip = mm(skip8[...], spread)[:1, :]
        x, g = x_v[j].astype(F32), g_v[j].astype(F32)
        xw = x * f
        later = later_v[j]
        lh, ll = two(later)
        q = (mm(b_ref[...], lh, 1, 1) + mm(b_ref[...], ll, 1, 1)) * end
        zq = z_v[j] + q
        dx_v[j] = (f * zq + skip * g).astype(BF16)
        pltpu.make_async_copy(dx_v.at[j], dx_hbm.at[:, columns(j)], dx_sem.at[j]).start()
        r_acc[...] += seg(x * zq, ones)
        eh, el = two(xw * end)
        db_ref[...] += mm(eh, lh) + mm(el, lh) + mm(eh, ll)
        p0, p1, p2 = three(chunk_start(j) * later)
        one8 = jnp.ones((8, STATES), BF16)
        dots = mm(one8, p0, 1, 1) + mm(one8, p1, 1, 1) + mm(one8, p2, 1, 1)
        at_end = jnp.sum(xw * q, axis=0, keepdims=True) + end * dots
        row_acc[...] += seg(jnp.where(iota((8, CHUNK), 0) == 0, at_end, 0.0), ones)

    def arrive_step(k, _):
        from_k = ORDER(k)
        j = gz.flat(from_k, -1)

        @pl.when(k > 0)
        def _():
            gz.copy(from_k, out6.at[0], later_v.at[0], sems, 5).wait()

        later_step(j)
        return 0

    lax.fori_loop(0, 8, arrive_step, 0)

    last = iota((SPAN, 128), 0) == SPAN - 1
    dcum = a_acc[...] - small[2] * r_acc[...] + jnp.where(last, row_acc[0:1, :], 0.0)
    up = tri(False)
    q0, q1, q2 = three(dcum)
    rc = mm(up, q0) + mm(up, q1) + mm(up, q2)
    rate = jnp.exp(four(decay_ref[...]))
    draw = (small[1] * r_acc[...] - rate * rc) * small[3]
    pd = jnp.sum(rc * small[0], axis=0, keepdims=True) * -rate
    pb = jnp.sum(draw, axis=0, keepdims=True)
    lane = iota((1, 128), 1) // HEADS
    total = jnp.where(lane == 0, pd, jnp.where(lane == 1, pb, jnp.where(lane == 2, row_acc[1:2, :], 0.0)))
    block[0] = total
    near = zc.send(lambda i: block.at[0], rec_a, (send_a, recv_a), 0)
    rec_a[zc.me] = total
    draw_ref[...] = draw.T[:HEADS, :]
    wait_all(near)
    total = jnp.sum(rec_a[...], axis=0)
    block[1] = total
    far = xy.send(lambda i: block.at[1], rec_b, (send_b, recv_b), 0)
    rec_b[xy.me] = total
    for j in range(8):
        pltpu.make_async_copy(dx_v.at[j], dx_hbm.at[:, columns(j)], dx_sem.at[j]).wait()
    wait_all(far)
    sums_ref[...] = jnp.broadcast_to(jnp.sum(rec_b[...], axis=0), (8, 128))


def ORDER(k):
    return (k % 4) * 2 + k // 4


def local(x, raw, b, c, decay, bias, skip, checkpoints, g):
    vmem, hbm = pl.BlockSpec(memory_space=pltpu.VMEM), pl.BlockSpec(memory_space=pltpu.HBM)
    buf = lambda *shape: pltpu.VMEM(shape, F32)
    half = lambda *shape: pltpu.VMEM(shape, BF16)
    dma = lambda *shape: pltpu.SemaphoreType.DMA(shape)
    row = lambda v: v.reshape(1, HEADS)
    keep = lambda v: pltpu.with_memory_space_constraint(v, pltpu.HBM)
    dx, draw, db, dc, sums = pl.pallas_call(
        kernel,
        out_shape=(
            jax.ShapeDtypeStruct((SPAN, HEADS * WIDTH), BF16),
            jax.ShapeDtypeStruct((HEADS, SPAN), F32),
            jax.ShapeDtypeStruct((SPAN, STATES), F32),
            jax.ShapeDtypeStruct((SPAN, STATES), F32),
            jax.ShapeDtypeStruct((8, 128), F32),
        ),
        in_specs=[hbm, vmem, vmem, vmem, hbm, hbm, hbm, hbm, hbm],
        out_specs=(hbm, vmem, vmem, vmem, vmem),
        scratch_shapes=[
            buf(HEADS, SPAN), half(SPAN, STATES), half(SPAN, STATES),
            half(8, SPAN, CHUNK), half(8, SPAN, CHUNK), half(8, SPAN, CHUNK), half(8, SPAN, CHUNK),
            half(8, SPAN, CHUNK), buf(8, SPAN, CHUNK), half(SPAN, 128), half(SPAN, 128), half(8, 128),
            buf(4, SPAN, 128), half(SPAN, SPAN), half(SPAN, SPAN), half(SPAN, SPAN), half(SPAN, SPAN),
            buf(SPAN, SPAN), buf(SPAN, 128), buf(SPAN, 128), buf(8, 128),
            buf(8, CHUNK + 8, STATES), buf(8, CHUNK + 8, STATES), buf(8, CHUNK, STATES), buf(8, 8, STATES),
            buf(8, PIECE + 8, STATES), buf(8, PIECE + 8, STATES), buf(8, PIECE, STATES), buf(8, 8, STATES),
            buf(PIECE + 8, STATES), buf(8, PIECE + 8, STATES), buf(8, PIECE, STATES), buf(8, PIECE, STATES),
            buf(8, CHUNK, STATES), buf(8, CHUNK, STATES), half(8, HEADS, 8, STATES),
            buf(2, 1, 128), buf(16, 1, 128), buf(32, 1, 128),
            dma(3), dma(8), dma(8), dma(8), pltpu.SemaphoreType.DMA, dma(6, 8), dma(6, 8),
            dma(1, 16), dma(1, 16), dma(1, 32), dma(1, 32),
        ],
        compiler_params=pltpu.CompilerParams(collective_id=0, has_side_effects=True, vmem_limit_bytes=40 * 2**20),
        name="spans",
    )(keep(raw.T), row(bias), row(decay), row(skip), keep(b), keep(c), keep(x), keep(g), keep(checkpoints))
    sums = sums[0]
    return dx, draw.T, db, dc, sums[:HEADS], sums[HEADS : 2 * HEADS], sums[2 * HEADS : 3 * HEADS]


GX_GY_GZ = ("gx_0", "gx_1", "gy", "gz_0", "gz_1")


def solution(mesh):
    torus = Mesh(mesh.devices.reshape(4, 2, mesh.shape["gy"], 4, 2), GX_GY_GZ)
    wide = P(GX_GY_GZ, None)
    return jax.shard_map(
        local,
        mesh=torus,
        in_specs=(wide, wide, wide, wide, P(), P(), P(), P(GX_GY_GZ[:3], None, GX_GY_GZ[3:], None), wide),
        out_specs=(wide, wide, wide, wide, P(), P(), P()),
        check_vma=False,
    )
```
